32 devices in a mesh: wide: 8 (over z, y), narrow: 4 (over x, core).
Axes of the slice: x: 2, y: 2, z: 4, core: 2. Of those that a mesh axis runs over, the one named last changes fastest.
Arguments:
- checkpoint_slots: float32 [4, 2, 256, 4096], P('narrow', None, 'wide'), may hold values from 0 to 2
- owner_slot: int32 [2], replicated, may hold values from 0 to 3
- row_velocity: float32 [256, 4096], P('wide', 'narrow'), may hold values from -0.4 to 0.4
- column_velocity: float32 [256, 4096], P('wide', 'narrow'), may hold values from -0.4 to 0.4
- land_sea: int32 [256, 4096], P('wide', 'narrow'), may hold values 0 or 1
- layer_class: int32 [2], replicated, may hold values from 0 to 3
- class_speed: float32 [4], replicated, may hold values from 0.05 to 0.6
- final_adjoint: float32 [2, 256, 4096], P(None, 'wide', 'narrow'), may hold values from -6 to 6
- deposit_weight: float32 [256, 4096], P('wide', 'narrow'), may hold values from -6 to 6
Outputs:
- initial_adjoint: float32 [2, 256, 4096], P(None, 'wide', 'narrow')
The draws below stay inside these ranges and needn't reach their ends.
All inputs are finite; a program needn't handle non-finite values. No bound on the sum of `land_sea` on one device may be relied on, other than what follows from the above.
Results may differ from the reference program's by a relative error of at most 0.00002.
Values sent between devices are 32-bit elements; how exact they have to be, the bound alone decides.
A program may use at most 64 MiB of HBM per device.

```python
import math
import jax
import jax.numpy as jnp
from jax import lax

LAYERS = 2
CLASSES = 4
STEPS = 3
NX = 256
NY = 4096
N_NARROW = 4


def with_ends(values, rng, low, top_value):
    shape = values.shape
    spot = [jax.random.randint(jax.random.fold_in(rng, axis), (), 0, shape[axis]) for axis in range(len(shape))]
    values = values.at[tuple(spot)].set(low)
    longest = shape.index(max(shape))
    spot[longest] = (spot[longest] + 1) % shape[longest]
    return values.at[tuple(spot)].set(top_value)


def block_levels(stream_key, dims, pieces, smallest, largest):
    gain, own = 1.0, jax.random.fold_in(stream_key, 6)
    for dim, shards_of in pieces:
        draws = jnp.exp(jax.random.uniform(jax.random.fold_in(own, dim), (shards_of,), jnp.float32, smallest / len(pieces), largest / len(pieces)))
        gain = gain * jnp.repeat(draws, dims[dim] // shards_of).reshape([-1 if axis == dim else 1 for axis in range(len(dims))])
    return gain


def gaussian(stream_key, shape, spread, reach, cuts=(), kind=jnp.bfloat16):
    loudness = block_levels(stream_key, shape, cuts, -0.22, 0.18) if cuts else 1.0
    values = jax.random.normal(stream_key, shape, jnp.float32) * spread * loudness
    return jnp.minimum(jnp.maximum(values, -reach), reach).astype(kind)


def setup_inputs(seed: int = 0) -> dict:
    splits = jax.random.split(jax.random.key(seed), 10)
    return {
        "checkpoint_slots": jnp.clip(2.0 * jax.random.uniform(splits[0], (N_NARROW, LAYERS, NX, NY), jnp.float32) ** block_levels(splits[0], (N_NARROW, LAYERS, NX, NY), ((0, 4), (2, 8)), -0.2, 0.2), 0.0, 2.0),
        "owner_slot": jax.random.randint(splits[1], (LAYERS,), 0, N_NARROW).astype(jnp.int32),
        "row_velocity": jnp.clip(jax.random.uniform(splits[2], (NX, NY), jnp.float32, -0.4, 0.4) * block_levels(splits[2], (NX, NY), ((0, 8), (1, 4)), -0.4, 0.0), -0.4, 0.4),
        "column_velocity": jnp.clip(jax.random.uniform(splits[3], (NX, NY), jnp.float32, -0.4, 0.4) * block_levels(splits[3], (NX, NY), ((0, 8), (1, 4)), -0.4, 0.0), -0.4, 0.4),
        "land_sea": with_ends((jax.random.randint(splits[4], (NX, NY), 0, 8) < 7).astype(jnp.int32), jax.random.fold_in(splits[4], 1), 0, 1),
        "layer_class": jax.random.randint(splits[5], (LAYERS,), 0, CLASSES).astype(jnp.int32),
        "class_speed": jnp.clip(jnp.exp(jax.random.uniform(splits[6], (CLASSES,), jnp.float32, math.log(0.05), math.log(0.6))), 0.05, 0.6),
        "final_adjoint": gaussian(splits[7], (LAYERS, NX, NY), 1.0, 6.0, ((1, 8), (2, 4)), jnp.float32),
        "deposit_weight": gaussian(splits[8], (NX, NY), 1.0, 6.0, ((0, 8), (1, 4)), jnp.float32),
    }


def stencil_weights(velocity):
    forward_part = jnp.maximum(velocity, 0.0)
    backward_part = jnp.minimum(velocity, 0.0)
    fsquare = forward_part * forward_part
    bsquare = backward_part * backward_part
    return [0.5 * fsquare - 0.5 * forward_part, 2.0 * forward_part - fsquare, 0.5 * fsquare - 1.5 * forward_part + 0.5 * bsquare + 1.5 * backward_part, -2.0 * backward_part - bsquare, 0.5 * bsquare + 0.5 * backward_part]

def advect(padded, row_weights, column_weights):
    height = padded.shape[1]
    breadth = padded.shape[2]
    result = padded[:, 2:height - 2, 2:breadth - 2]
    for offset in range(-2, 3):
        row_term = row_weights[offset + 2][2:height - 2, 2:breadth - 2]
        column_term = column_weights[offset + 2][2:height - 2, 2:breadth - 2]
        result = result + row_term * padded[:, 2 + offset:height - 2 + offset, 2:breadth - 2]
        result = result + column_term * padded[:, 2:height - 2, 2 + offset:breadth - 2 + offset]
    return result

def settle(advected, speeds, sea_mask):
    flux = speeds[:, None, None] * advected / (1.0 + advected * advected)
    above = jnp.concatenate([jnp.zeros_like(flux[:1]), flux[:-1]], 0)
    return ((advected - flux + above) * sea_mask, flux[-1] * sea_mask)

def layer_speeds(layer_class, class_speed):
    classes = jnp.arange(class_speed.shape[0], dtype=jnp.int32)
    return lax.optimization_barrier(jnp.sum(jnp.where(layer_class[:, None] == classes[None, :], class_speed[None, :], 0.0), axis=1))

def reference(checkpoint_slots, owner_slot, row_velocity, column_velocity, land_sea, layer_class, class_speed, final_adjoint, deposit_weight):
    slot_ids = jnp.arange(checkpoint_slots.shape[0], dtype=jnp.int32)
    chosen = owner_slot.astype(jnp.int32)[None, :, None, None] == slot_ids[:, None, None, None]
    start_state = lax.optimization_barrier(jnp.sum(jnp.where(chosen, checkpoint_slots, 0.0), axis=0))
    speeds = layer_speeds(layer_class, class_speed)
    sea_mask = land_sea.astype(jnp.float32)
    row_weights = stencil_weights(jnp.pad(row_velocity, 2))
    column_weights = stencil_weights(jnp.pad(column_velocity, 2))

    def forward(current):
        deposit = jnp.zeros_like(sea_mask)
        for step_index in range(STEPS):
            padded = jnp.pad(current, ((0, 0), (2, 2), (2, 2)))
            advected = advect(padded, row_weights, column_weights)
            current, bottom = settle(advected, speeds, sea_mask)
            deposit = deposit + bottom
        return (current, deposit)
    unused, pullback = jax.vjp(forward, start_state)
    initial, = pullback((final_adjoint, deposit_weight))
    return initial
```

```python
import functools

import jax
import jax.numpy as jnp
from jax import lax
from jax.experimental import pallas as pl
from jax.experimental.pallas import tpu as pltpu
from jax.sharding import PartitionSpec as P

STEPS = 3
RIM = 2
LANES = 128
ROWS = 8
MESH = pl.DeviceIdType.MESH


def stencil_weights(velocity):
    p = jnp.maximum(velocity, 0.0)
    q = jnp.minimum(velocity, 0.0)
    pp = p * p
    qq = q * q
    return [
        0.5 * pp - 0.5 * p,
        2.0 * p - pp,
        0.5 * pp - 1.5 * p + 0.5 * qq + 1.5 * q,
        -2.0 * q - qq,
        0.5 * qq + 0.5 * q,
    ]


def kernel(
    group_wide,
    group,
    owner_ref,
    class_ref,
    speed_ref,
    slots_ref,
    row_velocity_ref,
    column_velocity_ref,
    sea_ref,
    final_ref,
    deposit_ref,
    out_ref,
    near,
    mixed,
    far,
    field,
    slope,
    grad,
    wr,
    wc,
    centre,
    sea,
    row_send,
    row_recv,
    col_send,
    col_recv,
    near_sems,
    far_sems,
    halo_send_sems,
    halo_recv_sems,
):
    layers, height, breadth = out_ref.shape
    offsets = (-2, -1, 1, 2)
    pair = 2 if group % 2 == 0 else 1
    chips = group // pair
    w = lax.axis_index("wide")
    n = lax.axis_index("narrow")
    chip = lax.div(n, pair)
    core = lax.rem(n, pair)
    blocks = [(slice(r, r + ROWS), r) for r in range(0, height, ROWS)]

    has = {
        ("row", 0): w > 0,
        ("row", 1): w < group_wide - 1,
        ("col", 0): n > 0,
        ("col", 1): n < group - 1,
    }

    barrier = pltpu.get_barrier_semaphore()
    for side in (0, 1):
        @pl.when(has["row", side])
        def _():
            pl.semaphore_signal(
                barrier, inc=1, device_id=(w + (2 * side - 1), n), device_id_type=MESH
            )
    for by in range(1, group):
        pl.semaphore_signal(
            barrier, inc=1, device_id=(w, lax.rem(n + by, group)), device_id_type=MESH
        )
    pads = jnp.zeros((ROWS, breadth), jnp.float32)
    bottom_pad = slice(height + ROWS, height + 2 * ROWS)
    for k in range(layers):
        grad[k, 0:ROWS, :] = pads
        grad[k, bottom_pad, :] = pads
    for t in range(4):
        wr[t, 0:ROWS, :] = pads
        wr[t, bottom_pad, :] = pads
    arrivals = (
        group - 1 + has["row", 0].astype(jnp.int32) + has["row", 1].astype(jnp.int32)
    )
    pl.semaphore_wait(barrier, arrivals)

    def own(device):
        return slots_ref.at[0, :, :, pl.ds(pl.multiple_of(device * breadth, LANES), breadth)]

    order = [lax.rem(chip + by, chips) for by in range(1, chips)] + [chip]

    def near_copy(step):
        partner = chip * pair + (pair - 1 - core)
        target = order[step] * pair + (pair - 1 - core)
        return pltpu.make_async_remote_copy(
            src_ref=own(target),
            dst_ref=near.at[step],
            send_sem=near_sems.at[0, step],
            recv_sem=near_sems.at[1, step],
            device_id=(w, partner),
            device_id_type=MESH,
        )

    def far_copy(step, k):
        return pltpu.make_async_remote_copy(
            src_ref=mixed.at[step, k],
            dst_ref=far.at[step, k],
            send_sem=far_sems.at[0, step, k],
            recv_sem=far_sems.at[1, step, k],
            device_id=(w, order[step] * pair + core),
            device_id_type=MESH,
        )

    if pair == 2:
        for step in range(chips):
            near_copy(step).start()
    partner_slot = chip * pair + (pair - 1 - core)

    def chosen(step, k, rows):
        start = pl.multiple_of((order[step] * pair + core) * breadth, LANES)
        value = slots_ref[0, k, rows, pl.ds(start, breadth)]
        if pair == 2:
            value = jnp.where(owner_ref[k] == n, value, near[step, k, rows, :])
        return value

    for step in range(chips - 1):
        if pair == 2:
            near_copy(step).wait_recv()
        for k in range(layers):
            for rows, _r in blocks:
                mixed[step, k, rows, :] = chosen(step, k, rows)
            far_copy(step, k).start()

    speeds = []
    for k in range(layers):
        total = 0.0
        for c in range(speed_ref.shape[0]):
            total = jnp.where(class_ref[k] == c, speed_ref[c], total)
        speeds.append(total)

    for rows, r in blocks:
        inner = slice(ROWS + r, 2 * ROWS + r)
        row_w = stencil_weights(row_velocity_ref[rows, :])
        col_w = stencil_weights(column_velocity_ref[rows, :])
        for t, offset in enumerate(offsets):
            wr[t, inner, :] = row_w[offset + 2]
            wc[t, rows, :] = col_w[offset + 2]
        centre[rows, :] = 1.0 + row_w[2] + col_w[2]
        sea[rows, :] = sea_ref[rows, :].astype(jnp.float32)

    if pair == 2:
        near_copy(chips - 1).wait_recv()
    for k in range(layers):
        for step in range(chips - 1):
            far_copy(step, k).wait_recv()
        for rows, r in blocks:
            value = chosen(chips - 1, k, rows)
            for step in range(chips - 1):
                sender = lax.rem(chip + chips - 1 - step, chips)
                value = jnp.where(
                    lax.div(owner_ref[k], pair) == sender, far[step, k, rows, :], value
                )
            field[0, k, ROWS + r : 2 * ROWS + r, :] = value

    def halo_copies(turn):
        copies = {}
        for side in (0, 1):
            by = 2 * side - 1
            copies["row", side] = pltpu.make_async_remote_copy(
                src_ref=row_send.at[turn, side],
                dst_ref=row_recv.at[turn, side],
                send_sem=halo_send_sems.at[turn, side],
                recv_sem=halo_recv_sems.at[turn, side],
                device_id=(w + by, n),
                device_id_type=MESH,
            )
            if turn < STEPS:
                edge = slice(0, LANES) if side == 0 else slice(breadth - LANES, breadth)
                source = field.at[turn, :, ROWS : ROWS + height, edge]
            else:
                source = col_send.at[turn - STEPS, side]
            copies["col", side] = pltpu.make_async_remote_copy(
                src_ref=source,
                dst_ref=col_recv.at[turn, side],
                send_sem=halo_send_sems.at[turn, 2 + side],
                recv_sem=halo_recv_sems.at[turn, 2 + side],
                device_id=(w, n + by),
                device_id_type=MESH,
            )
        return copies

    def send_halo(turn):
        for (kind, side), copy in halo_copies(turn).items():
            pl.when(has[kind, side])(copy.start)

    def receive_halo(turn):
        for (kind, side), copy in halo_copies(turn).items():
            pl.when(has[kind, 1 - side])(copy.wait_recv)

    def ghost(side, kind):
        return has[kind, 1 - side]

    for turn in range(STEPS):
        for k in range(layers):
            rim = slice(k * RIM, (k + 1) * RIM)
            row_send[turn, 0, rim, :] = field[turn, k, ROWS : ROWS + RIM, :]
            row_send[turn, 1, rim, :] = field[turn, k, ROWS + height - RIM : ROWS + height, :]
        send_halo(turn)
        receive_halo(turn)
        for k in range(layers):
            rim = slice(k * RIM, (k + 1) * RIM)
            field[turn, k, ROWS - RIM : ROWS, :] = jnp.where(
                ghost(1, "row"), row_recv[turn, 1, rim, :], 0.0
            )
            field[turn, k, ROWS + height : ROWS + height + RIM, :] = jnp.where(
                ghost(0, "row"), row_recv[turn, 0, rim, :], 0.0
            )
        for rows, r in blocks:
            above = None
            for k in range(layers):
                base = ROWS + r
                here = field[turn, k, base : base + ROWS, :]
                wide = jnp.concatenate(
                    [
                        jnp.where(ghost(1, "col"), col_recv[turn, 1, k, rows, :], 0.0),
                        here,
                        jnp.where(ghost(0, "col"), col_recv[turn, 0, k, rows, :], 0.0),
                    ],
                    axis=1,
                )
                adv = centre[rows, :] * here
                for t, o in enumerate(offsets):
                    adv += wr[t, base : base + ROWS, :] * field[turn, k, base + o : base + o + ROWS, :]
                    moved = pltpu.roll(wide, (-o) % wide.shape[1], 1)
                    adv += wc[t, rows, :] * moved[:, LANES : LANES + breadth]
                square = adv * adv
                part = 1.0 / (1.0 + square)
                slope[turn, k, rows, :] = speeds[k] * (1.0 - square) * part * part
                if turn + 1 < STEPS:
                    flux = speeds[k] * adv * part
                    left = adv - flux
                    if above is not None:
                        left = left + above
                    field[turn + 1, k, base : base + ROWS, :] = left * sea[rows, :]
                    above = flux

    for turn in range(STEPS, 2 * STEPS):
        back = turn - STEPS
        step = STEPS - 1 - back
        adjoint = final_ref if back == 0 else out_ref
        for rows, r in blocks:
            base = ROWS + r
            mask = sea[rows, :]
            below = mask * deposit_ref[rows, :]
            for k in reversed(range(layers)):
                masked = adjoint[k, rows, :] * mask
                g = masked + (below - masked) * slope[step, k, rows, :]
                below = masked
                grad[k, base : base + ROWS, :] = g
                wall = jnp.zeros((ROWS, LANES), jnp.float32)
                gathered = None
                for t, o in enumerate(offsets):
                    product = jnp.concatenate([wall, wc[t, rows, :] * g, wall], axis=1)
                    moved = pltpu.roll(product, o % product.shape[1], 1)
                    gathered = moved if gathered is None else gathered + moved
                col_send[back, 0, k, rows, :] = gathered[:, :LANES]
                col_send[back, 1, k, rows, :] = gathered[:, LANES + breadth :]
                out_ref[k, rows, :] = gathered[:, LANES : LANES + breadth] + centre[rows, :] * g
        for k in range(layers):
            rim = slice(k * RIM, (k + 1) * RIM)
            for side, signs, at in ((0, (0, 1), ROWS - RIM), (1, (2, 3), ROWS + height)):
                total = None
                for t in signs:
                    o = offsets[t]
                    spot = slice(at - o, at - o + RIM)
                    term = wr[t, spot, :] * grad[k, spot, :]
                    total = term if total is None else total + term
                row_send[turn, side, rim, :] = total
        send_halo(turn)
        for k in range(layers):
            for rows, r in blocks:
                total = out_ref[k, rows, :]
                for t, o in enumerate(offsets):
                    spot = slice(ROWS + r - o, 2 * ROWS + r - o)
                    total += wr[t, spot, :] * grad[k, spot, :]
                out_ref[k, rows, :] = total
        receive_halo(turn)
        for k in range(layers):
            rim = slice(k * RIM, (k + 1) * RIM)
            out_ref[k, 0:RIM, :] += jnp.where(
                ghost(1, "row"), row_recv[turn, 1, rim, :], 0.0
            )
            out_ref[k, height - RIM : height, :] += jnp.where(
                ghost(0, "row"), row_recv[turn, 0, rim, :], 0.0
            )
            out_ref[k, :, 0:LANES] += jnp.where(
                ghost(1, "col"), col_recv[turn, 1, k], 0.0
            )
            out_ref[k, :, breadth - LANES : breadth] += jnp.where(
                ghost(0, "col"), col_recv[turn, 0, k], 0.0
            )

    if pair == 2:
        for step in range(chips):
            near_copy(step).wait_send()
    for step in range(chips - 1):
        for k in range(layers):
            far_copy(step, k).wait_send()
    for turn in range(2 * STEPS):
        for (kind, side), copy in halo_copies(turn).items():
            pl.when(has[kind, side])(copy.wait_send)


def body(group_wide, group, slots, owner, row_v, col_v, land_sea, layer_class, speed, final, deposit):
    layers, height, breadth = final.shape
    pair = 2 if group % 2 == 0 else 1
    chips = group // pair
    f32 = jnp.float32
    padded = height + 2 * ROWS
    vmem = pl.BlockSpec(memory_space=pltpu.VMEM)
    smem = pl.BlockSpec(memory_space=pltpu.SMEM)
    turns = 2 * STEPS
    return pl.pallas_call(
        functools.partial(kernel, group_wide, group),
        out_shape=jax.ShapeDtypeStruct(final.shape, f32),
        in_specs=[smem] * 3 + [vmem] * 6,
        out_specs=vmem,
        scratch_shapes=[
            pltpu.VMEM((chips, layers, height, breadth), f32),
            pltpu.VMEM((max(chips - 1, 1), layers, height, breadth), f32),
            pltpu.VMEM((max(chips - 1, 1), layers, height, breadth), f32),
            pltpu.VMEM((STEPS, layers, padded, breadth), f32),
            pltpu.VMEM((STEPS, layers, height, breadth), f32),
            pltpu.VMEM((layers, padded, breadth), f32),
            pltpu.VMEM((4, padded, breadth), f32),
            pltpu.VMEM((4, height, breadth), f32),
            pltpu.VMEM((height, breadth), f32),
            pltpu.VMEM((height, breadth), f32),
            pltpu.VMEM((turns, 2, layers * RIM, breadth), f32),
            pltpu.VMEM((turns, 2, layers * RIM, breadth), f32),
            pltpu.VMEM((STEPS, 2, layers, height, LANES), f32),
            pltpu.VMEM((turns, 2, layers, height, LANES), f32),
            pltpu.SemaphoreType.DMA((2, chips)),
            pltpu.SemaphoreType.DMA((2, max(chips - 1, 1), layers)),
            pltpu.SemaphoreType.DMA((turns, 4)),
            pltpu.SemaphoreType.DMA((turns, 4)),
        ],
        compiler_params=pltpu.CompilerParams(
            collective_id=0, has_side_effects=True, vmem_limit_bytes=48 * 1024 * 1024
        ),
    )(owner, layer_class, speed, slots, row_v, col_v, land_sea, final, deposit)


def solution(mesh):
    in_specs = (
        P("narrow", None, "wide", None),
        P(),
        P("wide", "narrow"),
        P("wide", "narrow"),
        P("wide", "narrow"),
        P(),
        P(),
        P(None, "wide", "narrow"),
        P("wide", "narrow"),
    )
    out_specs = P(None, "wide", "narrow")
    return jax.shard_map(
        functools.partial(body, mesh.shape["wide"], mesh.shape["narrow"]),
        mesh=mesh,
        in_specs=in_specs,
        out_specs=out_specs,
        check_vma=False,
    )
```

```python
import functools

import jax
import jax.numpy as jnp
from jax import lax
from jax.experimental import pallas as pl
from jax.experimental.pallas import tpu as pltpu
from jax.sharding import PartitionSpec as P

STEPS = 3
RIM = 2
LANES = 128
ROWS = 8
MESH = pl.DeviceIdType.MESH


def stencil_weights(velocity):
    p = jnp.maximum(velocity, 0.0)
    q = jnp.minimum(velocity, 0.0)
    pp = p * p
    qq = q * q
    return [
        0.5 * pp - 0.5 * p,
        2.0 * p - pp,
        0.5 * pp - 1.5 * p + 0.5 * qq + 1.5 * q,
        -2.0 * q - qq,
        0.5 * qq + 0.5 * q,
    ]


def kernel(
    group_wide,
    group,
    owner_hbm,
    class_hbm,
    speed_hbm,
    slots_ref,
    row_velocity_hbm,
    column_velocity_hbm,
    sea_hbm,
    final_hbm,
    deposit_hbm,
    out_ref,
    owner_ref,
    class_ref,
    speed_ref,
    row_velocity_ref,
    column_velocity_ref,
    sea_ref,
    final_ref,
    deposit_ref,
    mine,
    load_sems,
    mine_sems,
    near,
    mixed,
    far,
    field,
    slope,
    grad,
    wr,
    wc,
    centre,
    sea,
    row_send,
    row_recv,
    col_send,
    col_recv,
    near_sems,
    far_sems,
    halo_send_sems,
    halo_recv_sems,
):
    layers, height, breadth = out_ref.shape
    offsets = (-2, -1, 1, 2)
    pair = 2 if group % 2 == 0 else 1
    chips = group // pair
    w = lax.axis_index("wide")
    n = lax.axis_index("narrow")
    chip = lax.div(n, pair)
    core = lax.rem(n, pair)
    blocks = [(slice(r, r + ROWS), r) for r in range(0, height, ROWS)]

    has = {
        ("row", 0): w > 0,
        ("row", 1): w < group_wide - 1,
        ("col", 0): n > 0,
        ("col", 1): n < group - 1,
    }

    order = [lax.rem(chip + by, chips) for by in range(1, chips)] + [chip]

    def own(device):
        return slots_ref.at[0, :, :, pl.ds(pl.multiple_of(device * breadth, LANES), breadth)]

    mine_loads = [
        pltpu.make_async_copy(own(order[step] * pair + core), mine.at[step], mine_sems.at[step])
        for step in range(chips)
    ]
    loads = [
        pltpu.make_async_copy(source, target, load_sems.at[i])
        for i, (source, target) in enumerate(
            [
                (owner_hbm, owner_ref),
                (class_hbm, class_ref),
                (speed_hbm, speed_ref),
                (row_velocity_hbm, row_velocity_ref),
                (column_velocity_hbm, column_velocity_ref),
                (sea_hbm, sea_ref),
                (final_hbm, final_ref),
                (deposit_hbm, deposit_ref),
            ]
        )
    ]
    barrier = pltpu.get_barrier_semaphore()
    for side in (0, 1):
        @pl.when(has["row", side])
        def _():
            pl.semaphore_signal(
                barrier, inc=1, device_id=(w + (2 * side - 1), n), device_id_type=MESH
            )
    for by in range(1, group):
        pl.semaphore_signal(
            barrier, inc=1, device_id=(w, lax.rem(n + by, group)), device_id_type=MESH
        )
    loads[0].start()
    for load in mine_loads:
        load.start()
    for load in loads[1:]:
        load.start()
    pads = jnp.zeros((ROWS, breadth), jnp.float32)
    bottom_pad = slice(height + ROWS, height + 2 * ROWS)
    for k in range(layers):
        grad[k, 0:ROWS, :] = pads
        grad[k, bottom_pad, :] = pads
    for t in range(4):
        wr[t, 0:ROWS, :] = pads
        wr[t, bottom_pad, :] = pads
    arrivals = (
        group - 1 + has["row", 0].astype(jnp.int32) + has["row", 1].astype(jnp.int32)
    )
    pl.semaphore_wait(barrier, arrivals)

    def near_copy(step):
        partner = chip * pair + (pair - 1 - core)
        target = order[step] * pair + (pair - 1 - core)
        return pltpu.make_async_remote_copy(
            src_ref=own(target),
            dst_ref=near.at[step],
            send_sem=near_sems.at[0, step],
            recv_sem=near_sems.at[1, step],
            device_id=(w, partner),
            device_id_type=MESH,
        )

    def far_copy(step, k):
        return pltpu.make_async_remote_copy(
            src_ref=mixed.at[step, k],
            dst_ref=far.at[step, k],
            send_sem=far_sems.at[0, step, k],
            recv_sem=far_sems.at[1, step, k],
            device_id=(w, order[step] * pair + core),
            device_id_type=MESH,
        )

    if pair == 2:
        for step in range(chips):
            near_copy(step).start()
    partner_slot = chip * pair + (pair - 1 - core)

    def chosen(step, k, rows):
        value = mine[step, k, rows, :]
        if pair == 2:
            value = jnp.where(owner_ref[k] == n, value, near[step, k, rows, :])
        return value

    loads[0].wait()
    for step in range(chips - 1):
        mine_loads[step].wait()
        if pair == 2:
            near_copy(step).wait_recv()
        for k in range(layers):
            for rows, _r in blocks:
                mixed[step, k, rows, :] = chosen(step, k, rows)
            far_copy(step, k).start()

    for load in loads[1:]:
        load.wait()
    speeds = []
    for k in range(layers):
        total = 0.0
        for c in range(speed_ref.shape[0]):
            total = jnp.where(class_ref[k] == c, speed_ref[c], total)
        speeds.append(total)

    for rows, r in blocks:
        inner = slice(ROWS + r, 2 * ROWS + r)
        row_w = stencil_weights(row_velocity_ref[rows, :])
        col_w = stencil_weights(column_velocity_ref[rows, :])
        for t, offset in enumerate(offsets):
            wr[t, inner, :] = row_w[offset + 2]
            wc[t, rows, :] = col_w[offset + 2]
        centre[rows, :] = 1.0 + row_w[2] + col_w[2]
        sea[rows, :] = sea_ref[rows, :].astype(jnp.float32)

    mine_loads[chips - 1].wait()
    if pair == 2:
        near_copy(chips - 1).wait_recv()
    for k in range(layers):
        for step in range(chips - 1):
            far_copy(step, k).wait_recv()
        for rows, r in blocks:
            value = chosen(chips - 1, k, rows)
            for step in range(chips - 1):
                sender = lax.rem(chip + chips - 1 - step, chips)
                value = jnp.where(
                    lax.div(owner_ref[k], pair) == sender, far[step, k, rows, :], value
                )
            field[0, k, ROWS + r : 2 * ROWS + r, :] = value

    def halo_copies(turn):
        copies = {}
        for side in (0, 1):
            by = 2 * side - 1
            copies["row", side] = pltpu.make_async_remote_copy(
                src_ref=row_send.at[turn, side],
                dst_ref=row_recv.at[turn, side],
                send_sem=halo_send_sems.at[turn, side],
                recv_sem=halo_recv_sems.at[turn, side],
                device_id=(w + by, n),
                device_id_type=MESH,
            )
            if turn < STEPS:
                edge = slice(0, LANES) if side == 0 else slice(breadth - LANES, breadth)
                source = field.at[turn, :, ROWS : ROWS + height, edge]
            else:
                source = col_send.at[turn - STEPS, side]
            copies["col", side] = pltpu.make_async_remote_copy(
                src_ref=source,
                dst_ref=col_recv.at[turn, side],
                send_sem=halo_send_sems.at[turn, 2 + side],
                recv_sem=halo_recv_sems.at[turn, 2 + side],
                device_id=(w, n + by),
                device_id_type=MESH,
            )
        return copies

    def send_halo(turn):
        for (kind, side), copy in halo_copies(turn).items():
            pl.when(has[kind, side])(copy.start)

    def receive_halo(turn):
        for (kind, side), copy in halo_copies(turn).items():
            pl.when(has[kind, 1 - side])(copy.wait_recv)

    def ghost(side, kind):
        return has[kind, 1 - side]

    for turn in range(STEPS):
        for k in range(layers):
            rim = slice(k * RIM, (k + 1) * RIM)
            row_send[turn, 0, rim, :] = field[turn, k, ROWS : ROWS + RIM, :]
            row_send[turn, 1, rim, :] = field[turn, k, ROWS + height - RIM : ROWS + height, :]
        send_halo(turn)
        receive_halo(turn)
        for k in range(layers):
            rim = slice(k * RIM, (k + 1) * RIM)
            field[turn, k, ROWS - RIM : ROWS, :] = jnp.where(
                ghost(1, "row"), row_recv[turn, 1, rim, :], 0.0
            )
            field[turn, k, ROWS + height : ROWS + height + RIM, :] = jnp.where(
                ghost(0, "row"), row_recv[turn, 0, rim, :], 0.0
            )
        for rows, r in blocks:
            above = None
            for k in range(layers):
                base = ROWS + r
                here = field[turn, k, base : base + ROWS, :]
                wide = jnp.concatenate(
                    [
                        jnp.where(ghost(1, "col"), col_recv[turn, 1, k, rows, :], 0.0),
                        here,
                        jnp.where(ghost(0, "col"), col_recv[turn, 0, k, rows, :], 0.0),
                    ],
                    axis=1,
                )
                adv = centre[rows, :] * here
                for t, o in enumerate(offsets):
                    adv += wr[t, base : base + ROWS, :] * field[turn, k, base + o : base + o + ROWS, :]
                    moved = pltpu.roll(wide, (-o) % wide.shape[1], 1)
                    adv += wc[t, rows, :] * moved[:, LANES : LANES + breadth]
                square = adv * adv
                part = 1.0 / (1.0 + square)
                slope[turn, k, rows, :] = speeds[k] * (1.0 - square) * part * part
                if turn + 1 < STEPS:
                    flux = speeds[k] * adv * part
                    left = adv - flux
                    if above is not None:
                        left = left + above
                    field[turn + 1, k, base : base + ROWS, :] = left * sea[rows, :]
                    above = flux

    for turn in range(STEPS, 2 * STEPS):
        back = turn - STEPS
        step = STEPS - 1 - back
        adjoint = final_ref if back == 0 else out_ref
        for rows, r in blocks:
            base = ROWS + r
            mask = sea[rows, :]
            below = mask * deposit_ref[rows, :]
            for k in reversed(range(layers)):
                masked = adjoint[k, rows, :] * mask
                g = masked + (below - masked) * slope[step, k, rows, :]
                below = masked
                grad[k, base : base + ROWS, :] = g
                wall = jnp.zeros((ROWS, LANES), jnp.float32)
                gathered = None
                for t, o in enumerate(offsets):
                    product = jnp.concatenate([wall, wc[t, rows, :] * g, wall], axis=1)
                    moved = pltpu.roll(product, o % product.shape[1], 1)
                    gathered = moved if gathered is None else gathered + moved
                col_send[back, 0, k, rows, :] = gathered[:, :LANES]
                col_send[back, 1, k, rows, :] = gathered[:, LANES + breadth :]
                out_ref[k, rows, :] = gathered[:, LANES : LANES + breadth] + centre[rows, :] * g
        for k in range(layers):
            rim = slice(k * RIM, (k + 1) * RIM)
            for side, signs, at in ((0, (0, 1), ROWS - RIM), (1, (2, 3), ROWS + height)):
                total = None
                for t in signs:
                    o = offsets[t]
                    spot = slice(at - o, at - o + RIM)
                    term = wr[t, spot, :] * grad[k, spot, :]
                    total = term if total is None else total + term
                row_send[turn, side, rim, :] = total
        send_halo(turn)
        for k in range(layers):
            for rows, r in blocks:
                total = out_ref[k, rows, :]
                for t, o in enumerate(offsets):
                    spot = slice(ROWS + r - o, 2 * ROWS + r - o)
                    total += wr[t, spot, :] * grad[k, spot, :]
                out_ref[k, rows, :] = total
        receive_halo(turn)
        for k in range(layers):
            rim = slice(k * RIM, (k + 1) * RIM)
            out_ref[k, 0:RIM, :] += jnp.where(
                ghost(1, "row"), row_recv[turn, 1, rim, :], 0.0
            )
            out_ref[k, height - RIM : height, :] += jnp.where(
                ghost(0, "row"), row_recv[turn, 0, rim, :], 0.0
            )
            out_ref[k, :, 0:LANES] += jnp.where(
                ghost(1, "col"), col_recv[turn, 1, k], 0.0
            )
            out_ref[k, :, breadth - LANES : breadth] += jnp.where(
                ghost(0, "col"), col_recv[turn, 0, k], 0.0
            )

    if pair == 2:
        for step in range(chips):
            near_copy(step).wait_send()
    for step in range(chips - 1):
        for k in range(layers):
            far_copy(step, k).wait_send()
    for turn in range(2 * STEPS):
        for (kind, side), copy in halo_copies(turn).items():
            pl.when(has[kind, side])(copy.wait_send)


def body(group_wide, group, slots, owner, row_v, col_v, land_sea, layer_class, speed, final, deposit):
    layers, height, breadth = final.shape
    pair = 2 if group % 2 == 0 else 1
    chips = group // pair
    f32 = jnp.float32
    padded = height + 2 * ROWS
    vmem = pl.BlockSpec(memory_space=pltpu.VMEM)
    hbm = pl.BlockSpec(memory_space=pltpu.HBM)
    turns = 2 * STEPS
    return pl.pallas_call(
        functools.partial(kernel, group_wide, group),
        out_shape=jax.ShapeDtypeStruct(final.shape, f32),
        in_specs=[hbm] * 9,
        out_specs=vmem,
        scratch_shapes=[
            pltpu.SMEM(owner.shape, owner.dtype),
            pltpu.SMEM(layer_class.shape, layer_class.dtype),
            pltpu.SMEM(speed.shape, speed.dtype),
            pltpu.VMEM(row_v.shape, f32),
            pltpu.VMEM(col_v.shape, f32),
            pltpu.VMEM(land_sea.shape, land_sea.dtype),
            pltpu.VMEM(final.shape, f32),
            pltpu.VMEM(deposit.shape, f32),
            pltpu.VMEM((chips, layers, height, breadth), f32),
            pltpu.SemaphoreType.DMA((8,)),
            pltpu.SemaphoreType.DMA((chips,)),
            pltpu.VMEM((chips, layers, height, breadth), f32),
            pltpu.VMEM((max(chips - 1, 1), layers, height, breadth), f32),
            pltpu.VMEM((max(chips - 1, 1), layers, height, breadth), f32),
            pltpu.VMEM((STEPS, layers, padded, breadth), f32),
            pltpu.VMEM((STEPS, layers, height, breadth), f32),
            pltpu.VMEM((layers, padded, breadth), f32),
            pltpu.VMEM((4, padded, breadth), f32),
            pltpu.VMEM((4, height, breadth), f32),
            pltpu.VMEM((height, breadth), f32),
            pltpu.VMEM((height, breadth), f32),
            pltpu.VMEM((turns, 2, layers * RIM, breadth), f32),
            pltpu.VMEM((turns, 2, layers * RIM, breadth), f32),
            pltpu.VMEM((STEPS, 2, layers, height, LANES), f32),
            pltpu.VMEM((turns, 2, layers, height, LANES), f32),
            pltpu.SemaphoreType.DMA((2, chips)),
            pltpu.SemaphoreType.DMA((2, max(chips - 1, 1), layers)),
            pltpu.SemaphoreType.DMA((turns, 4)),
            pltpu.SemaphoreType.DMA((turns, 4)),
        ],
        compiler_params=pltpu.CompilerParams(
            collective_id=0, has_side_effects=True, vmem_limit_bytes=67043328
        ),
    )(owner, layer_class, speed, slots, row_v, col_v, land_sea, final, deposit)


def solution(mesh):
    in_specs = (
        P("narrow", None, "wide", None),
        P(),
        P("wide", "narrow"),
        P("wide", "narrow"),
        P("wide", "narrow"),
        P(),
        P(),
        P(None, "wide", "narrow"),
        P("wide", "narrow"),
    )
    out_specs = P(None, "wide", "narrow")
    return jax.shard_map(
        functools.partial(body, mesh.shape["wide"], mesh.shape["narrow"]),
        mesh=mesh,
        in_specs=in_specs,
        out_specs=out_specs,
        check_vma=False,
    )
```

```python
import functools

import jax
import jax.numpy as jnp
from jax import lax
from jax.experimental import pallas as pl
from jax.experimental.pallas import tpu as pltpu
from jax.sharding import PartitionSpec as P

STEPS = 3
RIM = 2
LANES = 128
ROWS = 8
MESH = pl.DeviceIdType.MESH


def stencil_weights(velocity):
    p = jnp.maximum(velocity, 0.0)
    q = jnp.minimum(velocity, 0.0)
    pp = p * p
    qq = q * q
    return [
        0.5 * pp - 0.5 * p,
        2.0 * p - pp,
        0.5 * pp - 1.5 * p + 0.5 * qq + 1.5 * q,
        -2.0 * q - qq,
        0.5 * qq + 0.5 * q,
    ]


def kernel(
    group_wide,
    group,
    owner_hbm,
    class_hbm,
    speed_hbm,
    slots_ref,
    row_velocity_hbm,
    column_velocity_hbm,
    sea_hbm,
    final_hbm,
    deposit_hbm,
    out_ref,
    owner_ref,
    class_ref,
    speed_ref,
    row_velocity_ref,
    column_velocity_ref,
    sea_ref,
    final_ref,
    deposit_ref,
    mine,
    load_sems,
    mine_sems,
    near,
    mixed,
    far,
    field,
    slope,
    grad,
    wr,
    wc,
    centre,
    sea,
    row_send,
    row_recv,
    col_send,
    col_recv,
    near_sems,
    far_sems,
    halo_send_sems,
    halo_recv_sems,
):
    layers, height, breadth = out_ref.shape
    offsets = (-2, -1, 1, 2)
    pair = 2 if group % 2 == 0 else 1
    chips = group // pair
    w = lax.axis_index("wide")
    n = lax.axis_index("narrow")
    chip = lax.div(n, pair)
    core = lax.rem(n, pair)
    blocks = [(slice(r, r + ROWS), r) for r in range(0, height, ROWS)]

    has = {
        ("row", 0): w > 0,
        ("row", 1): w < group_wide - 1,
        ("col", 0): n > 0,
        ("col", 1): n < group - 1,
    }

    order = [lax.rem(chip + by, chips) for by in range(1, chips)] + [chip]

    def own(device):
        return slots_ref.at[0, :, :, pl.ds(pl.multiple_of(device * breadth, LANES), breadth)]

    mine_loads = [
        pltpu.make_async_copy(own(order[step] * pair + core), mine.at[step], mine_sems.at[step])
        for step in range(chips)
    ]
    loads = [
        pltpu.make_async_copy(source, target, load_sems.at[i])
        for i, (source, target) in enumerate(
            [
                (owner_hbm, owner_ref),
                (class_hbm, class_ref),
                (speed_hbm, speed_ref),
                (row_velocity_hbm, row_velocity_ref),
                (column_velocity_hbm, column_velocity_ref),
                (sea_hbm, sea_ref),
                (final_hbm, final_ref),
                (deposit_hbm, deposit_ref),
            ]
        )
    ]
    barrier = pltpu.get_barrier_semaphore()
    for side in (0, 1):
        @pl.when(has["row", side])
        def _():
            pl.semaphore_signal(
                barrier, inc=1, device_id=(w + (2 * side - 1), n), device_id_type=MESH
            )
    for by in range(1, group):
        pl.semaphore_signal(
            barrier, inc=1, device_id=(w, lax.rem(n + by, group)), device_id_type=MESH
        )
    loads[0].start()
    for load in mine_loads:
        load.start()
    for load in loads[1:]:
        load.start()
    pads = jnp.zeros((ROWS, breadth), jnp.float32)
    bottom_pad = slice(height + ROWS, height + 2 * ROWS)
    for k in range(layers):
        grad[k, 0:ROWS, :] = pads
        grad[k, bottom_pad, :] = pads
    for t in range(4):
        wr[t, 0:ROWS, :] = pads
        wr[t, bottom_pad, :] = pads
    arrivals = (
        group - 1 + has["row", 0].astype(jnp.int32) + has["row", 1].astype(jnp.int32)
    )
    pl.semaphore_wait(barrier, arrivals)

    def near_copy(step):
        partner = chip * pair + (pair - 1 - core)
        target = order[step] * pair + (pair - 1 - core)
        return pltpu.make_async_remote_copy(
            src_ref=own(target),
            dst_ref=near.at[step],
            send_sem=near_sems.at[0, step],
            recv_sem=near_sems.at[1, step],
            device_id=(w, partner),
            device_id_type=MESH,
        )

    def far_copy(step, k):
        return pltpu.make_async_remote_copy(
            src_ref=mixed.at[step, k],
            dst_ref=far.at[step, k],
            send_sem=far_sems.at[0, step, k],
            recv_sem=far_sems.at[1, step, k],
            device_id=(w, order[step] * pair + core),
            device_id_type=MESH,
        )

    if pair == 2:
        for step in range(chips):
            near_copy(step).start()
    partner_slot = chip * pair + (pair - 1 - core)

    def chosen(step, k, rows):
        value = mine[step, k, rows, :]
        if pair == 2:
            value = jnp.where(owner_ref[k] == n, value, near[step, k, rows, :])
        return value

    loads[0].wait()
    for step in range(chips - 1):
        mine_loads[step].wait()
        if pair == 2:
            near_copy(step).wait_recv()
        for k in range(layers):
            for rows, _r in blocks:
                mixed[step, k, rows, :] = chosen(step, k, rows)
            far_copy(step, k).start()

    for load in loads[1:]:
        load.wait()
    speeds = []
    for k in range(layers):
        total = 0.0
        for c in range(speed_ref.shape[0]):
            total = jnp.where(class_ref[k] == c, speed_ref[c], total)
        speeds.append(total)

    for rows, r in blocks:
        inner = slice(ROWS + r, 2 * ROWS + r)
        row_w = stencil_weights(row_velocity_ref[rows, :])
        col_w = stencil_weights(column_velocity_ref[rows, :])
        for t, offset in enumerate(offsets):
            wr[t, inner, :] = row_w[offset + 2]
            wc[t, rows, :] = col_w[offset + 2]
        centre[rows, :] = 1.0 + row_w[2] + col_w[2]
        sea[rows, :] = sea_ref[rows, :].astype(jnp.float32)

    mine_loads[chips - 1].wait()
    if pair == 2:
        near_copy(chips - 1).wait_recv()
    for k in range(layers):
        for step in range(chips - 1):
            far_copy(step, k).wait_recv()
        for rows, r in blocks:
            value = chosen(chips - 1, k, rows)
            for step in range(chips - 1):
                sender = lax.rem(chip + chips - 1 - step, chips)
                value = jnp.where(
                    lax.div(owner_ref[k], pair) == sender, far[step, k, rows, :], value
                )
            field[0, k, ROWS + r : 2 * ROWS + r, :] = value

    def halo_copies(turn):
        copies = {}
        for side in (0, 1):
            by = 2 * side - 1
            copies["row", side] = pltpu.make_async_remote_copy(
                src_ref=row_send.at[turn, side],
                dst_ref=row_recv.at[turn, side],
                send_sem=halo_send_sems.at[turn, side],
                recv_sem=halo_recv_sems.at[turn, side],
                device_id=(w + by, n),
                device_id_type=MESH,
            )
            if turn < STEPS:
                edge = slice(0, LANES) if side == 0 else slice(breadth - LANES, breadth)
                source = field.at[turn, :, ROWS : ROWS + height, edge]
            else:
                source = col_send.at[turn - STEPS, side]
            copies["col", side] = pltpu.make_async_remote_copy(
                src_ref=source,
                dst_ref=col_recv.at[turn, side],
                send_sem=halo_send_sems.at[turn, 2 + side],
                recv_sem=halo_recv_sems.at[turn, 2 + side],
                device_id=(w, n + by),
                device_id_type=MESH,
            )
        return copies

    def send_halo(turn, which):
        for (kind, side), copy in halo_copies(turn).items():
            if kind == which:
                pl.when(has[kind, side])(copy.start)

    def send_field_rows(turn):
        for k in range(layers):
            rim = slice(k * RIM, (k + 1) * RIM)
            row_send[turn, 0, rim, :] = field[turn, k, ROWS : ROWS + RIM, :]
            row_send[turn, 1, rim, :] = field[turn, k, ROWS + height - RIM : ROWS + height, :]
        send_halo(turn, "row")

    def send_grad_rows(turn):
        for k in range(layers):
            rim = slice(k * RIM, (k + 1) * RIM)
            for side, signs, at in ((0, (0, 1), ROWS - RIM), (1, (2, 3), ROWS + height)):
                total = None
                for t in signs:
                    o = offsets[t]
                    spot = slice(at - o, at - o + RIM)
                    term = wr[t, spot, :] * grad[k, spot, :]
                    total = term if total is None else total + term
                row_send[turn, side, rim, :] = total
        send_halo(turn, "row")

    edges = blocks[:1] + blocks[1:][-1:]
    edges_first = edges + blocks[1:-1]

    def receive_halo(turn):
        for (kind, side), copy in halo_copies(turn).items():
            pl.when(has[kind, 1 - side])(copy.wait_recv)

    def ghost(side, kind):
        return has[kind, 1 - side]

    send_field_rows(0)
    for turn in range(STEPS):
        send_halo(turn, "col")
        receive_halo(turn)
        for k in range(layers):
            rim = slice(k * RIM, (k + 1) * RIM)
            field[turn, k, ROWS - RIM : ROWS, :] = jnp.where(
                ghost(1, "row"), row_recv[turn, 1, rim, :], 0.0
            )
            field[turn, k, ROWS + height : ROWS + height + RIM, :] = jnp.where(
                ghost(0, "row"), row_recv[turn, 0, rim, :], 0.0
            )
        for i, (rows, r) in enumerate(edges_first):
            above = None
            for k in range(layers):
                base = ROWS + r
                here = field[turn, k, base : base + ROWS, :]
                wide = jnp.concatenate(
                    [
                        jnp.where(ghost(1, "col"), col_recv[turn, 1, k, rows, :], 0.0),
                        here,
                        jnp.where(ghost(0, "col"), col_recv[turn, 0, k, rows, :], 0.0),
                    ],
                    axis=1,
                )
                adv = centre[rows, :] * here
                for t, o in enumerate(offsets):
                    adv += wr[t, base : base + ROWS, :] * field[turn, k, base + o : base + o + ROWS, :]
                    moved = pltpu.roll(wide, (-o) % wide.shape[1], 1)
                    adv += wc[t, rows, :] * moved[:, LANES : LANES + breadth]
                square = adv * adv
                part = 1.0 / (1.0 + square)
                slope[turn, k, rows, :] = speeds[k] * (1.0 - square) * part * part
                if turn + 1 < STEPS:
                    flux = speeds[k] * adv * part
                    left = adv - flux
                    if above is not None:
                        left = left + above
                    field[turn + 1, k, base : base + ROWS, :] = left * sea[rows, :]
                    above = flux
            if turn + 1 < STEPS and i + 1 == len(edges):
                send_field_rows(turn + 1)

    for turn in range(STEPS, 2 * STEPS):
        back = turn - STEPS
        step = STEPS - 1 - back
        adjoint = final_ref if back == 0 else out_ref
        for i, (rows, r) in enumerate(edges_first):
            base = ROWS + r
            mask = sea[rows, :]
            below = mask * deposit_ref[rows, :]
            for k in reversed(range(layers)):
                masked = adjoint[k, rows, :] * mask
                g = masked + (below - masked) * slope[step, k, rows, :]
                below = masked
                grad[k, base : base + ROWS, :] = g
                wall = jnp.zeros((ROWS, LANES), jnp.float32)
                gathered = None
                for t, o in enumerate(offsets):
                    product = jnp.concatenate([wall, wc[t, rows, :] * g, wall], axis=1)
                    moved = pltpu.roll(product, o % product.shape[1], 1)
                    gathered = moved if gathered is None else gathered + moved
                col_send[back, 0, k, rows, :] = gathered[:, :LANES]
                col_send[back, 1, k, rows, :] = gathered[:, LANES + breadth :]
                out_ref[k, rows, :] = gathered[:, LANES : LANES + breadth] + centre[rows, :] * g
            if i + 1 == len(edges):
                send_grad_rows(turn)
        send_halo(turn, "col")
        for k in range(layers):
            for rows, r in blocks:
                total = out_ref[k, rows, :]
                for t, o in enumerate(offsets):
                    spot = slice(ROWS + r - o, 2 * ROWS + r - o)
                    total += wr[t, spot, :] * grad[k, spot, :]
                out_ref[k, rows, :] = total
        receive_halo(turn)
        for k in range(layers):
            rim = slice(k * RIM, (k + 1) * RIM)
            out_ref[k, 0:RIM, :] += jnp.where(
                ghost(1, "row"), row_recv[turn, 1, rim, :], 0.0
            )
            out_ref[k, height - RIM : height, :] += jnp.where(
                ghost(0, "row"), row_recv[turn, 0, rim, :], 0.0
            )
            out_ref[k, :, 0:LANES] += jnp.where(
                ghost(1, "col"), col_recv[turn, 1, k], 0.0
            )
            out_ref[k, :, breadth - LANES : breadth] += jnp.where(
                ghost(0, "col"), col_recv[turn, 0, k], 0.0
            )

    if pair == 2:
        for step in range(chips):
            near_copy(step).wait_send()
    for step in range(chips - 1):
        for k in range(layers):
            far_copy(step, k).wait_send()
    for turn in range(2 * STEPS):
        for (kind, side), copy in halo_copies(turn).items():
            pl.when(has[kind, side])(copy.wait_send)


def body(group_wide, group, slots, owner, row_v, col_v, land_sea, layer_class, speed, final, deposit):
    layers, height, breadth = final.shape
    pair = 2 if group % 2 == 0 else 1
    chips = group // pair
    f32 = jnp.float32
    padded = height + 2 * ROWS
    vmem = pl.BlockSpec(memory_space=pltpu.VMEM)
    hbm = pl.BlockSpec(memory_space=pltpu.HBM)
    turns = 2 * STEPS
    return pl.pallas_call(
        functools.partial(kernel, group_wide, group),
        out_shape=jax.ShapeDtypeStruct(final.shape, f32),
        in_specs=[hbm] * 9,
        out_specs=vmem,
        scratch_shapes=[
            pltpu.SMEM(owner.shape, owner.dtype),
            pltpu.SMEM(layer_class.shape, layer_class.dtype),
            pltpu.SMEM(speed.shape, speed.dtype),
            pltpu.VMEM(row_v.shape, f32),
            pltpu.VMEM(col_v.shape, f32),
            pltpu.VMEM(land_sea.shape, land_sea.dtype),
            pltpu.VMEM(final.shape, f32),
            pltpu.VMEM(deposit.shape, f32),
            pltpu.VMEM((chips, layers, height, breadth), f32),
            pltpu.SemaphoreType.DMA((8,)),
            pltpu.SemaphoreType.DMA((chips,)),
            pltpu.VMEM((chips, layers, height, breadth), f32),
            pltpu.VMEM((max(chips - 1, 1), layers, height, breadth), f32),
            pltpu.VMEM((max(chips - 1, 1), layers, height, breadth), f32),
            pltpu.VMEM((STEPS, layers, padded, breadth), f32),
            pltpu.VMEM((STEPS, layers, height, breadth), f32),
            pltpu.VMEM((layers, padded, breadth), f32),
            pltpu.VMEM((4, padded, breadth), f32),
            pltpu.VMEM((4, height, breadth), f32),
            pltpu.VMEM((height, breadth), f32),
            pltpu.VMEM((height, breadth), f32),
            pltpu.VMEM((turns, 2, layers * RIM, breadth), f32),
            pltpu.VMEM((turns, 2, layers * RIM, breadth), f32),
            pltpu.VMEM((STEPS, 2, layers, height, LANES), f32),
            pltpu.VMEM((turns, 2, layers, height, LANES), f32),
            pltpu.SemaphoreType.DMA((2, chips)),
            pltpu.SemaphoreType.DMA((2, max(chips - 1, 1), layers)),
            pltpu.SemaphoreType.DMA((turns, 4)),
            pltpu.SemaphoreType.DMA((turns, 4)),
        ],
        compiler_params=pltpu.CompilerParams(
            collective_id=0, has_side_effects=True, vmem_limit_bytes=67043328
        ),
    )(owner, layer_class, speed, slots, row_v, col_v, land_sea, final, deposit)


def solution(mesh):
    in_specs = (
        P("narrow", None, "wide", None),
        P(),
        P("wide", "narrow"),
        P("wide", "narrow"),
        P("wide", "narrow"),
        P(),
        P(),
        P(None, "wide", "narrow"),
        P("wide", "narrow"),
    )
    out_specs = P(None, "wide", "narrow")
    return jax.shard_map(
        functools.partial(body, mesh.shape["wide"], mesh.shape["narrow"]),
        mesh=mesh,
        in_specs=in_specs,
        out_specs=out_specs,
        check_vma=False,
    )
```
